32 devices in a mesh: dom: 16 (over z, y, x), field: 2 (over core).
Axes of the slice: x: 2, y: 2, z: 4, core: 2. Of those that a mesh axis runs over, the one named last changes fastest.
Arguments:
- ocean: bfloat16 [30, 32768], P('field', 'dom'), may hold values from -6 to 6
- grad_weight: bfloat16 [256, 4, 128, 256], P('dom'), may hold values from -0.25 to 0.25
- neighbours: int32 [256, 4], P('dom'), may hold values from 0 to 255, as said below
- remap_weight: bfloat16 [2048, 384, 128], P(('dom', 'field')), may hold values from -0.109375 to 0.109375
- tile_src: int32 [2048], P(('dom', 'field')), may hold values from 0 to 255, as said below
- tile_atm: int32 [2048], P(('dom', 'field')), may hold values from 0 to 255, as said below
- atm_owner: int32 [256], replicated, may hold values from 0 to 255, as said below
Outputs:
- atmosphere: float32 [30, 32768], P('field', 'dom')
The draws below stay inside these ranges and needn't reach their ends.
Inputs may be any that keep to these rules, and one draw needn't show every extreme that they name: `neighbours`: the stencil of a block of partition p holds blocks of p, the last 2 blocks of partition p - 1 or the first 2 blocks of partition p + 1 (partitions are the aligned runs of 16 blocks; no wrap). `tile_src`: tile t names a block of partition t // 128, the partition that holds the tile. `tile_atm`: of the aligned runs of 64 tiles, no run has more than 16 tiles whose atmosphere tile has owner position in one aligned run of 16; in every draw each run reaches 16 for some owner. `atm_owner`: A permutation of the atmosphere tiles.
All inputs are finite; a program needn't handle non-finite values.
Results may differ from the reference program's by a relative error of at most 0.0042.
Values may be sent and summed in bfloat16 or wider, within the bound.
A program may use at most 64 MiB of HBM per device.

```python
import jax
import jax.numpy as jnp
from jax import lax

F = 30
BLK = 128
ACELL = 128
K = 4
NH = 2
NB = 16
TPC = 64
AT = 16
NBLK = 256
TILES = 2048
ATILES = 256
N_FIELD = 2


def routing(key):
    owner_key, pick_key, heat_key, slot_key = jax.random.split(jax.random.fold_in(key, 7), 4)
    atm_owner = jax.random.permutation(owner_key, ATILES).astype(jnp.int32)
    inverse = jnp.argsort(atm_owner).astype(jnp.int32)
    devices = ATILES // AT
    cores = TILES // TPC
    capacity = max(2, 4 * TPC // devices)
    groups = TPC // capacity
    heat = jax.random.randint(heat_key, (devices,), 0, 3)
    noise = jax.random.randint(pick_key, (cores, devices), 0, 1024)
    scores = (noise + 512 * heat[None, :]) * devices + jnp.arange(devices)[None, :]
    _, chosen = lax.top_k(scores, groups)
    target = jnp.repeat(chosen, capacity, axis=1)
    local_slot = jax.random.randint(slot_key, (cores, TPC), 0, AT)
    slots = (target * AT + local_slot).reshape(TILES).astype(jnp.int32)
    return (atm_owner, inverse[slots].astype(jnp.int32))


def draw_atm_owner(key, part):
    return routing(key)[0]


def draw_tile_atm(key, part):
    return routing(key)[1]


def draw_tile_src(key, part):
    devices = NBLK // NB
    per_device = TILES // devices
    device = jnp.arange(TILES) // per_device
    offset = jax.random.randint(jax.random.fold_in(key, 5), (TILES,), 0, NB)
    return (device * NB + offset).astype(jnp.int32)


def draw_neighbours(key, part):
    block_ids = jnp.arange(NBLK)[:, None]
    device = block_ids // NB
    pick = jax.random.randint(jax.random.fold_in(key, 3), (NBLK, K), 0, NB + 2 * NH)
    before = (device - 1) * NB + NB - NH + pick
    inside = device * NB + pick - NH
    after = (device + 1) * NB + pick - NH - NB
    chosen = jnp.where(pick < NH, before, jnp.where(pick < NH + NB, inside, after))
    own_block = device * NB + pick % NB
    outside = (chosen < 0) | (chosen >= NBLK)
    return jnp.where(outside, own_block, chosen).astype(jnp.int32)


def level_of(rng, dims, shards, least, largest):
    level = 1.0
    for axis_at, parts in shards:
        heights = jax.random.uniform(jax.random.fold_in(jax.random.fold_in(rng, 6), axis_at), (parts,), jnp.float32, least / len(shards), largest / len(shards))
        level = level * jnp.repeat(jnp.exp(heights), dims[axis_at] // parts).reshape((-1,) + (1,) * (len(dims) - 1 - axis_at))
    return level


def normal_values(rng, extent, deviation, bound, cuts=(), dtype=jnp.bfloat16):
    result = deviation * jax.random.normal(rng, extent, jnp.float32)
    if cuts:
        result = result * level_of(rng, extent, cuts, -0.22, 0.18)
    return jnp.clip(result, -bound, bound).astype(dtype)


def setup_inputs(seed: int = 0) -> dict:
    streams_of = jax.random.split(jax.random.key(seed), 8)
    ocean = normal_values(streams_of[0], (F, NBLK * BLK), 1.0, 6.0, ((0, 2), (1, 16)))
    grad_weight = normal_values(streams_of[1], (NBLK, K, BLK, 2 * BLK), (K * BLK) ** -0.5, 0.25, ((0, 16),))
    neighbours = draw_neighbours(jax.random.fold_in(streams_of[7], 71), 0)
    remap_weight = normal_values(streams_of[3], (TILES, 3 * BLK, ACELL), (3 * BLK * TPC * N_FIELD // AT) ** -0.5, 0.109375, ((0, 32),))
    tile_src = draw_tile_src(jax.random.fold_in(streams_of[7], 71), 0)
    tile_atm = draw_tile_atm(jax.random.fold_in(streams_of[7], 71), 0)
    atm_owner = draw_atm_owner(jax.random.fold_in(streams_of[7], 71), 0)
    return dict(ocean=ocean, grad_weight=grad_weight, neighbours=neighbours, remap_weight=remap_weight, tile_src=tile_src, tile_atm=tile_atm, atm_owner=atm_owner)


def reference(ocean, grad_weight, neighbours, remap_weight, tile_src, tile_atm, atm_owner):
    fields = ocean.shape[0]
    blocks = ocean.reshape(fields, NBLK, BLK)
    picked = blocks[:, neighbours]
    grouped_vals = picked.reshape(fields, NBLK // NB, NB, K, BLK).transpose(1, 0, 2, 3, 4)
    grouped_weights = grad_weight.reshape(NBLK // NB, NB, K, BLK, 2 * BLK)

    def gradient_group(pieces):
        group_vals, group_weights = pieces
        return jnp.einsum('fbkj,bkjo->fbo', group_vals.astype(jnp.float32), group_weights.astype(jnp.float32))

    gradient = lax.map(gradient_group, (grouped_vals, grouped_weights))
    gradient = gradient.transpose(1, 0, 2, 3).reshape(fields, NBLK, 2 * BLK).astype(jnp.bfloat16)
    source = jnp.concatenate([blocks, gradient], axis=2)
    atm_slot = atm_owner[tile_atm].astype(jnp.int32)
    groups = TILES // TPC

    def add_group(summed, pieces):
        weights, src_ids, slots = pieces
        source_rows = source[:, src_ids].astype(jnp.float32)
        contribution = jnp.einsum('ftj,tjc->tfc', source_rows, weights.astype(jnp.float32), precision=lax.Precision.HIGHEST)
        return summed.at[slots].add(contribution), None

    initial = jnp.zeros((ATILES, fields, ACELL), jnp.float32)
    summed, _ = lax.scan(add_group, initial, (remap_weight.reshape(groups, TPC, 3 * BLK, ACELL), tile_src.reshape(groups, TPC), atm_slot.reshape(groups, TPC)))
    return summed.transpose(1, 0, 2).reshape(fields, ATILES * ACELL)
```

```python
import functools

import jax
import jax.numpy as jnp
from jax import lax
from jax.experimental import pallas as pl
from jax.experimental.pallas import tpu as pltpu
from jax.sharding import PartitionSpec as P


def padded_2(shard, sides, width):
    for axis, dim in sides:
        size, length = (lax.axis_size(axis), shard.shape[dim])
        up = [(i, (i + 1) % size) for i in range(size - 1)]
        down = [(j, i) for i, j in up]
        last = lax.slice_in_dim(shard, length - width, length, axis=dim)
        initial = lax.slice_in_dim(shard, 0, width, axis=dim)
        before = lax.ppermute(last, axis, up)
        after = lax.ppermute(initial, axis, down)
        shard = jnp.concatenate([before, shard, after], axis=dim)
    return shard


def deliver(contribution, target_dev, local_slot, devices, capacity, owned):
    tile_count = target_dev.shape[0]
    tile_order = jnp.arange(tile_count, dtype=jnp.int32)
    before = jnp.sum(
        (
            (target_dev[:, None] == target_dev[None, :])
            & (tile_order[None, :] < tile_order[:, None])
        ).astype(jnp.int32),
        axis=1,
    )
    position = target_dev * capacity + before
    slot_count = devices * capacity
    matches = position[None, :] == jnp.arange(slot_count, dtype=jnp.int32)[:, None]
    chosen = jnp.sum(jnp.where(matches, tile_order[None, :], 0), axis=1)
    filled = jnp.any(matches, axis=1)
    outgoing = jnp.where(filled[:, None, None], contribution[chosen], 0.0)
    targets = jnp.where(filled, local_slot[chosen], -1)
    incoming, in_targets = (
        lax.all_to_all(outgoing, "dom", split_axis=0, concat_axis=0, tiled=True),
        lax.all_to_all(targets, "dom", split_axis=0, concat_axis=0, tiled=True),
    )
    selector = (in_targets[None, :] == jnp.arange(owned, dtype=jnp.int32)[:, None]).astype(
        jnp.float32
    )
    summed = jnp.einsum("ak,kfc->fac", selector, incoming, precision=lax.Precision.HIGHEST)
    return summed.reshape(summed.shape[0], owned * summed.shape[2])


def local(ocean, grad_weight, neighbours, remap_weight, tile_src, tile_atm, atm_owner):
    block_len = grad_weight.shape[2]
    field_rows = ocean.shape[0]
    nblocks = grad_weight.shape[0]
    device = lax.axis_index("dom")
    devices = lax.axis_size("dom")
    per_core = tile_atm.shape[0]
    capacity_base = max(2, 4 * per_core // devices)
    padded = padded_2(ocean, (("dom", 1),), nblocks * block_len)
    first_block = device * nblocks - nblocks
    extended = padded.reshape(field_rows, -1, block_len)
    local_ids = neighbours - first_block
    picked = jnp.take(extended, local_ids, axis=1)
    gradient = jnp.einsum(
        "fbkj,bkjo->fbo", picked, grad_weight, preferred_element_type=jnp.float32
    ).astype(jnp.bfloat16)
    source = jnp.concatenate([ocean.reshape(field_rows, nblocks, block_len), gradient], axis=2)
    source = lax.all_gather(source, "field", axis=0, tiled=True)
    local_src = tile_src - device * nblocks
    source_rows = jnp.take(source, local_src, axis=1)
    contribution = jnp.einsum(
        "ftj,tjc->tfc", source_rows, remap_weight, preferred_element_type=jnp.float32
    )
    atm_tiles = atm_owner.shape[0]
    atm_slot = jnp.sum(
        jnp.where(
            tile_atm[:, None] == jnp.arange(atm_tiles, dtype=jnp.int32)[None, :],
            atm_owner[None, :],
            0,
        ),
        axis=1,
    )
    owned = atm_tiles // devices
    target_dev = atm_slot // owned
    local_slot = atm_slot % owned
    summed = deliver(contribution, target_dev, local_slot, devices, capacity_base, owned)
    return lax.psum_scatter(summed, "field", scatter_dimension=0, tiled=True)


HALO = 2
MESH = pl.DeviceIdType.MESH


def stage_masks(stages, core):
    masks = [jnp.int32(1 << s) for s in range(stages)]
    if stages >= 2:
        masks[0] = jnp.where(core == 0, 1, 2)
        masks[1] = jnp.where(core == 0, 2, 1)
    return masks


def fused_kernel(
    devices, stages, owned, groups,
    ocean, neighbours, tile_src, tile_atm, atm_owner, grad_weight, remap_weight,
    out,
    gw, rw, other, halo, other_atm, ext, source, own_part, send_part, recv_part,
    select, rhs, acc, outgoing, incoming, turned,
    gw_sem, rw_sem, near_send, near_recv, part_send, part_recv, red_send, red_recv,
):
    me, core = lax.axis_index("dom"), lax.axis_index("field")
    fields, width = ocean.shape
    nblocks, stencil, block_len, grad_len = gw.shape
    tiles, depth, cells = rw.shape
    rows = devices * owned
    span = fields // groups * cells
    peer = (me, 1 - core)
    gw_parts, rw_parts, c_parts = gw_sem.shape[0], rw_sem.shape[0], part_send.shape[0]
    gw_step, rw_step, c_step = nblocks // gw_parts, tiles // rw_parts, tiles // c_parts

    gw_copies = [
        pltpu.make_async_copy(
            grad_weight.at[pl.ds(i * gw_step, gw_step)],
            gw.at[pl.ds(i * gw_step, gw_step)],
            gw_sem.at[i],
        )
        for i in range(gw_parts)
    ]
    rw_copies = [
        pltpu.make_async_copy(
            remap_weight.at[pl.ds(i * rw_step, rw_step)],
            rw.at[pl.ds(i * rw_step, rw_step)],
            rw_sem.at[i],
        )
        for i in range(rw_parts)
    ]
    for copy in gw_copies + rw_copies:
        copy.start()

    masks = stage_masks(stages, core)
    has_left, has_right = me > 0, me < devices - 1
    barrier = pltpu.get_barrier_semaphore()

    def greet(target):
        pl.semaphore_signal(barrier, inc=1, device_id=target, device_id_type=MESH)

    greet(peer)
    for mask in masks:
        greet((me ^ mask, core))

    @pl.when(has_left)
    def _():
        greet((me - 1, core))
        greet((me - 1, 1 - core))

    @pl.when(has_right)
    def _():
        greet((me + 1, core))
        greet((me + 1, 1 - core))

    sides = jnp.minimum(me, 1) + jnp.minimum(devices - 1 - me, 1)
    pl.semaphore_wait(barrier, 1 + stages + 2 * sides)

    def remote(src, dst, send, recv, target):
        return pltpu.make_async_remote_copy(
            src_ref=src, dst_ref=dst, send_sem=send, recv_sem=recv,
            device_id=target, device_id_type=MESH,
        )

    edge = HALO * block_len
    first = ocean.at[:, pl.ds(0, edge)]
    last = ocean.at[:, pl.ds(width - edge, edge)]
    left_copies = [
        remote(first, halo.at[1, g], near_send.at[g], near_recv.at[2 + g], (me - 1, (core + g) % 2))
        for g in range(2)
    ]
    right_copies = [
        remote(last, halo.at[0, g], near_send.at[2 + g], near_recv.at[g], (me + 1, (core + g) % 2))
        for g in range(2)
    ]

    @pl.when(has_left)
    def _():
        for copy in left_copies:
            copy.start()

    @pl.when(has_right)
    def _():
        for copy in right_copies:
            copy.start()

    ocean_copy = remote(ocean, other, near_send.at[4], near_recv.at[4], peer)
    ocean_copy.start()
    atm_copy = remote(tile_atm, other_atm, near_send.at[5], near_recv.at[5], peer)
    atm_copy.start()

    half_rows = ext.shape[1] // 2

    def spread(data, block, group):
        low = group * half_rows
        ext[block, pl.ds(low, fields), :] = data

    for b in range(nblocks):
        spread(ocean[:, pl.ds(b * block_len, block_len)], HALO + b, 0)
    slot = atm_owner[...]
    away = (slot // owned) ^ me
    bits = [(away >> s) & 1 for s in range(stages)]
    if stages >= 2:
        zero, one = bits[0], bits[1]
        bits[0] = jnp.where(core == 0, zero, one)
        bits[1] = jnp.where(core == 0, one, zero)
    rank = bits[0] * 0
    for bit in bits:
        rank = rank * 2 + bit
    rel = rank * owned + slot % owned
    ocean_copy.wait_recv()
    for b in range(nblocks):
        spread(other[:, pl.ds(b * block_len, block_len)], HALO + b, 1)
    atm_copy.wait_recv()
    atm_tiles = atm_owner.shape[1]
    owner_hot = (lax.broadcasted_iota(jnp.int32, (rows, atm_tiles), 0) == rel).astype(
        jnp.float32
    ).astype(jnp.bfloat16)
    ids = lax.broadcasted_iota(jnp.int32, (atm_tiles, tiles), 0)
    tile_hot = jnp.concatenate(
        [
            (ids == tile_atm[...]).astype(jnp.float32),
            (ids == other_atm[...]).astype(jnp.float32),
        ],
        axis=1,
    ).astype(jnp.bfloat16)
    chosen = jnp.dot(owner_hot, tile_hot, preferred_element_type=jnp.float32)
    select[:, : 2 * tiles] = chosen.astype(jnp.bfloat16)
    select[:, 2 * tiles :] = chosen[:, :tiles].astype(jnp.bfloat16)

    @pl.when(has_right)
    def _():
        for g in range(2):
            left_copies[g].wait_recv()
            for b in range(HALO):
                spread(halo[1, g, :, pl.ds(b * block_len, block_len)], HALO + nblocks + b, g)

    @pl.when(has_left)
    def _():
        for g in range(2):
            right_copies[g].wait_recv()
            for b in range(HALO):
                spread(halo[0, g, :, pl.ds(b * block_len, block_len)], b, g)

    base = me * nblocks
    for i in range(gw_parts):
        gw_copies[i].wait()

        def gradient(j, _, i=i):
            b = i * gw_step + j
            picked = [ext[jnp.clip(neighbours[k, b] - base + HALO, 0, nblocks + 2 * HALO - 1)] for k in range(stencil)]
            weights = gw[b].reshape(stencil * block_len, grad_len)
            grad = jnp.dot(
                jnp.concatenate(picked, axis=1), weights, preferred_element_type=jnp.float32
            )
            source[b, :, :block_len] = ext[HALO + b]
            source[b, :, block_len:] = grad.astype(jnp.bfloat16)
            return 0

        lax.fori_loop(0, gw_step, gradient, 0, unroll=True)

    part_copies = []
    loads_per = rw_parts // c_parts
    for i in range(c_parts):
        for j in range(loads_per):
            rw_copies[i * loads_per + j].wait()

        def contribute(j, _, i=i):
            t = i * c_step + j
            value = jnp.dot(
                source[jnp.clip(tile_src[t] - base, 0, nblocks - 1)], rw[t], preferred_element_type=jnp.float32
            )
            own_part[pl.ds(t * half_rows, half_rows), :] = value[:half_rows]
            send_part[t] = value[half_rows:].astype(jnp.bfloat16)
            return 0

        lax.fori_loop(0, c_step, contribute, 0, unroll=8)
        copy = remote(
            send_part.at[pl.ds(i * c_step, c_step)],
            recv_part.at[pl.ds(i * c_step, c_step)],
            part_send.at[i], part_recv.at[i], peer,
        )
        copy.start()
        part_copies.append(copy)

    for f in range(fields):
        g, at = f // (fields // groups), f % (fields // groups)
        mine = own_part[pl.ds(f, tiles, stride=half_rows), :]
        high = mine.astype(jnp.bfloat16)
        low = (mine - high.astype(jnp.float32)).astype(jnp.bfloat16)
        rhs[g, :tiles, at * cells : (at + 1) * cells] = high
        rhs[g, 2 * tiles :, at * cells : (at + 1) * cells] = low
    for i in range(c_parts):
        part_copies[i].wait_recv()
        own_part[pl.ds((tiles + i * c_step) * half_rows, c_step * half_rows), :] = (
            recv_part[pl.ds(i * c_step, c_step)]
            .astype(jnp.float32)
            .reshape(c_step * half_rows, cells)
        )

    def reduction(g, s):
        part = rows >> (s + 1)
        return remote(
            outgoing.at[g, pl.ds(part, part)], incoming.at[g, pl.ds(part, part)],
            red_send.at[g, s], red_recv.at[g, s], (me ^ masks[s], core),
        )

    per = fields // groups
    for g in range(groups):
        for at in range(per):
            theirs = own_part[pl.ds(tiles * half_rows + g * per + at, tiles, stride=half_rows), :]
            rhs[g, tiles : 2 * tiles, at * cells : (at + 1) * cells] = theirs.astype(jnp.bfloat16)
        outgoing[g, rows // 2 :] = jnp.dot(
            select[rows // 2 :], rhs[g], preferred_element_type=jnp.float32
        ).astype(jnp.bfloat16)
        reduction(g, 0).start()
    for g in range(groups):
        acc[g] = jnp.dot(select[: rows // 2], rhs[g], preferred_element_type=jnp.float32)
    for s in range(stages):
        part = rows >> (s + 1)
        for g in range(groups):
            reduction(g, s).wait_recv()
            if s < stages - 1:
                quarter = part // 2
                outgoing[g, quarter:part] = (
                    acc[g, quarter:part] + incoming[g, part + quarter : 2 * part].astype(jnp.float32)
                ).astype(jnp.bfloat16)
                reduction(g, s + 1).start()
                acc[g, :quarter] += incoming[g, part : part + quarter].astype(jnp.float32)
            else:
                final = acc[g, :part] + incoming[g, part : 2 * part].astype(jnp.float32)
                for at in range(per):
                    turned[pl.ds((g * per + at) * owned, owned), :] = final[
                        :, at * cells : (at + 1) * cells
                    ]
    for a in range(owned):
        out[:, pl.ds(a * cells, cells)] = turned[pl.ds(a, fields, stride=owned), :]

    @pl.when(has_left)
    def _():
        for copy in left_copies:
            copy.wait_send()

    @pl.when(has_right)
    def _():
        for copy in right_copies:
            copy.wait_send()

    ocean_copy.wait_send()
    atm_copy.wait_send()
    for copy in part_copies:
        copy.wait_send()
    for s in range(stages):
        for g in range(groups):
            reduction(g, s).wait_send()


def fused(ocean, grad_weight, neighbours, remap_weight, tile_src, tile_atm, atm_owner):
    fields, width = ocean.shape
    devices = lax.axis_size("dom")
    stages = devices.bit_length() - 1
    nblocks, _, block_len, grad_len = grad_weight.shape
    tiles, depth, cells = remap_weight.shape
    owned = atm_owner.shape[0] // devices
    rows = devices * owned
    groups = 3 if fields % 3 == 0 else 1
    span = fields // groups * cells
    half = -(-fields // 16) * 16
    bf16, f32 = jnp.bfloat16, jnp.float32
    dma = pltpu.SemaphoreType.DMA
    vmem = pl.BlockSpec(memory_space=pltpu.VMEM)
    smem = pl.BlockSpec(memory_space=pltpu.SMEM)
    anyspace = pl.BlockSpec(memory_space=pl.ANY)
    return pl.pallas_call(
        functools.partial(fused_kernel, devices, stages, owned, groups),
        out_shape=jax.ShapeDtypeStruct((fields, owned * cells), f32),
        in_specs=[vmem, smem, smem, vmem, vmem, anyspace, anyspace],
        out_specs=vmem,
        scratch_shapes=[
            pltpu.VMEM(grad_weight.shape, bf16),
            pltpu.VMEM(remap_weight.shape, bf16),
            pltpu.VMEM((fields, width), bf16),
            pltpu.VMEM((2, 2, fields, HALO * block_len), bf16),
            pltpu.VMEM((1, tiles), jnp.int32),
            pltpu.VMEM((nblocks + 2 * HALO, 2 * half, block_len), bf16),
            pltpu.VMEM((nblocks, 2 * half, depth), bf16),
            pltpu.VMEM((2 * tiles * half, cells), f32),
            pltpu.VMEM((tiles, half, cells), bf16),
            pltpu.VMEM((tiles, half, cells), bf16),
            pltpu.VMEM((rows, 3 * tiles), bf16),
            pltpu.VMEM((groups, 3 * tiles, span), bf16),
            pltpu.VMEM((groups, rows // 2, span), f32),
            pltpu.VMEM((groups, rows, span), bf16),
            pltpu.VMEM((groups, rows, span), bf16),
            pltpu.VMEM((fields * owned, cells), f32),
            dma((4,)), dma((8,)), dma((6,)), dma((6,)), dma((4,)), dma((4,)),
            dma((groups, stages)), dma((groups, stages)),
        ],
        compiler_params=pltpu.CompilerParams(
            collective_id=0, has_side_effects=True, vmem_limit_bytes=60 * 2**20
        ),
    )(
        ocean, neighbours.T, tile_src, tile_atm.reshape(1, -1), atm_owner.reshape(1, -1),
        grad_weight, remap_weight,
    )


def plan(ocean, grad_weight, neighbours, remap_weight, tile_src, tile_atm, atm_owner):
    devices = lax.axis_size("dom")
    atm_tiles = atm_owner.shape[0]
    power = devices > 1 and devices & (devices - 1) == 0
    small = atm_tiles * ocean.shape[0] * remap_weight.shape[2] <= 2**20
    even = (atm_tiles // devices) % 16 == 0 and lax.axis_size("field") == 2
    body = fused if power and small and even else local
    return body(ocean, grad_weight, neighbours, remap_weight, tile_src, tile_atm, atm_owner)


def solution(mesh):
    in_specs = (
        P("field", "dom"),
        P("dom", None, None, None),
        P("dom", None),
        P(("dom", "field"), None, None),
        P(("dom", "field")),
        P(("dom", "field")),
        P(),
    )
    out_specs = P("field", "dom")
    return jax.shard_map(plan, mesh=mesh, in_specs=in_specs, out_specs=out_specs, check_vma=False)
```

```python
import functools

import jax
import jax.numpy as jnp
from jax import lax
from jax.experimental import pallas as pl
from jax.experimental.pallas import tpu as pltpu
from jax.sharding import PartitionSpec as P


def padded_2(shard, sides, width):
    for axis, dim in sides:
        size, length = (lax.axis_size(axis), shard.shape[dim])
        up = [(i, (i + 1) % size) for i in range(size - 1)]
        down = [(j, i) for i, j in up]
        last = lax.slice_in_dim(shard, length - width, length, axis=dim)
        initial = lax.slice_in_dim(shard, 0, width, axis=dim)
        before = lax.ppermute(last, axis, up)
        after = lax.ppermute(initial, axis, down)
        shard = jnp.concatenate([before, shard, after], axis=dim)
    return shard


def deliver(contribution, target_dev, local_slot, devices, capacity, owned):
    tile_count = target_dev.shape[0]
    tile_order = jnp.arange(tile_count, dtype=jnp.int32)
    before = jnp.sum(
        (
            (target_dev[:, None] == target_dev[None, :])
            & (tile_order[None, :] < tile_order[:, None])
        ).astype(jnp.int32),
        axis=1,
    )
    position = target_dev * capacity + before
    slot_count = devices * capacity
    matches = position[None, :] == jnp.arange(slot_count, dtype=jnp.int32)[:, None]
    chosen = jnp.sum(jnp.where(matches, tile_order[None, :], 0), axis=1)
    filled = jnp.any(matches, axis=1)
    outgoing = jnp.where(filled[:, None, None], contribution[chosen], 0.0)
    targets = jnp.where(filled, local_slot[chosen], -1)
    incoming, in_targets = (
        lax.all_to_all(outgoing, "dom", split_axis=0, concat_axis=0, tiled=True),
        lax.all_to_all(targets, "dom", split_axis=0, concat_axis=0, tiled=True),
    )
    selector = (in_targets[None, :] == jnp.arange(owned, dtype=jnp.int32)[:, None]).astype(
        jnp.float32
    )
    summed = jnp.einsum("ak,kfc->fac", selector, incoming, precision=lax.Precision.HIGHEST)
    return summed.reshape(summed.shape[0], owned * summed.shape[2])


def local(ocean, grad_weight, neighbours, remap_weight, tile_src, tile_atm, atm_owner):
    block_len = grad_weight.shape[2]
    field_rows = ocean.shape[0]
    nblocks = grad_weight.shape[0]
    device = lax.axis_index("dom")
    devices = lax.axis_size("dom")
    per_core = tile_atm.shape[0]
    capacity_base = max(2, 4 * per_core // devices)
    padded = padded_2(ocean, (("dom", 1),), nblocks * block_len)
    first_block = device * nblocks - nblocks
    extended = padded.reshape(field_rows, -1, block_len)
    local_ids = neighbours - first_block
    picked = jnp.take(extended, local_ids, axis=1)
    gradient = jnp.einsum(
        "fbkj,bkjo->fbo", picked, grad_weight, preferred_element_type=jnp.float32
    ).astype(jnp.bfloat16)
    source = jnp.concatenate([ocean.reshape(field_rows, nblocks, block_len), gradient], axis=2)
    source = lax.all_gather(source, "field", axis=0, tiled=True)
    local_src = tile_src - device * nblocks
    source_rows = jnp.take(source, local_src, axis=1)
    contribution = jnp.einsum(
        "ftj,tjc->tfc", source_rows, remap_weight, preferred_element_type=jnp.float32
    )
    atm_tiles = atm_owner.shape[0]
    atm_slot = jnp.sum(
        jnp.where(
            tile_atm[:, None] == jnp.arange(atm_tiles, dtype=jnp.int32)[None, :],
            atm_owner[None, :],
            0,
        ),
        axis=1,
    )
    owned = atm_tiles // devices
    target_dev = atm_slot // owned
    local_slot = atm_slot % owned
    summed = deliver(contribution, target_dev, local_slot, devices, capacity_base, owned)
    return lax.psum_scatter(summed, "field", scatter_dimension=0, tiled=True)


HALO = 2
MESH = pl.DeviceIdType.MESH


def stage_bits(stages, kind, core):
    order = list(range(stages))
    if kind == 1:
        order = [2, 0, 1] + order[3:]
    swapped = [{0: 1, 1: 0}.get(b, b) for b in order] if stages >= 2 else order
    return [jnp.where(core == 0, a, b) if a != b else a for a, b in zip(order, swapped)]


def kind_of(group, groups, stages):
    return 1 if group == 1 and groups > 2 and stages >= 3 else 0


def fused_kernel(
    devices, stages, owned, groups,
    ocean, neighbours, tile_src, tile_atm, atm_owner, grad_weight, remap_weight,
    out,
    gw, rw, other, halo, other_atm, ext, source, own_part, send_part, recv_part,
    select, rhs, acc, outgoing, incoming, turned,
    gw_sem, rw_sem, near_send, near_recv, part_send, part_recv, red_send, red_recv,
):
    me, core = lax.axis_index("dom"), lax.axis_index("field")
    fields, width = ocean.shape
    nblocks, stencil, block_len, grad_len = gw.shape
    tiles, depth, cells = rw.shape
    rows = devices * owned
    span = fields // groups * cells
    peer = (me, 1 - core)
    gw_parts, rw_parts, c_parts = gw_sem.shape[0], rw_sem.shape[0], part_send.shape[0]
    gw_step, rw_step, c_step = nblocks // gw_parts, tiles // rw_parts, tiles // c_parts

    gw_copies = [
        pltpu.make_async_copy(
            grad_weight.at[pl.ds(i * gw_step, gw_step)],
            gw.at[pl.ds(i * gw_step, gw_step)],
            gw_sem.at[i],
        )
        for i in range(gw_parts)
    ]
    rw_copies = [
        pltpu.make_async_copy(
            remap_weight.at[pl.ds(i * rw_step, rw_step)],
            rw.at[pl.ds(i * rw_step, rw_step)],
            rw_sem.at[i],
        )
        for i in range(rw_parts)
    ]
    for copy in gw_copies + rw_copies:
        copy.start()

    kinds = [kind_of(g, groups, stages) for g in range(groups)]
    bits_of = [stage_bits(stages, kind, core) for kind in range(max(kinds) + 1)]
    has_left, has_right = me > 0, me < devices - 1
    barrier = pltpu.get_barrier_semaphore()

    def greet(target):
        pl.semaphore_signal(barrier, inc=1, device_id=target, device_id_type=MESH)

    greet(peer)
    for s in range(stages):
        greet((me ^ (1 << s), core))

    @pl.when(has_left)
    def _():
        greet((me - 1, core))
        greet((me - 1, 1 - core))

    @pl.when(has_right)
    def _():
        greet((me + 1, core))
        greet((me + 1, 1 - core))

    sides = jnp.minimum(me, 1) + jnp.minimum(devices - 1 - me, 1)
    pl.semaphore_wait(barrier, 1 + stages + 2 * sides)

    def remote(src, dst, send, recv, target):
        return pltpu.make_async_remote_copy(
            src_ref=src, dst_ref=dst, send_sem=send, recv_sem=recv,
            device_id=target, device_id_type=MESH,
        )

    edge = HALO * block_len
    first = ocean.at[:, pl.ds(0, edge)]
    last = ocean.at[:, pl.ds(width - edge, edge)]
    left_copies = [
        remote(first, halo.at[1, g], near_send.at[g], near_recv.at[2 + g], (me - 1, (core + g) % 2))
        for g in range(2)
    ]
    right_copies = [
        remote(last, halo.at[0, g], near_send.at[2 + g], near_recv.at[g], (me + 1, (core + g) % 2))
        for g in range(2)
    ]

    @pl.when(has_left)
    def _():
        for copy in left_copies:
            copy.start()

    @pl.when(has_right)
    def _():
        for copy in right_copies:
            copy.start()

    ocean_copy = remote(ocean, other, near_send.at[4], near_recv.at[4], peer)
    ocean_copy.start()
    atm_copy = remote(tile_atm, other_atm, near_send.at[5], near_recv.at[5], peer)
    atm_copy.start()

    half_rows = ext.shape[1] // 2

    def spread(data, block, group):
        low = group * half_rows
        ext[block, pl.ds(low, fields), :] = data

    for b in range(nblocks):
        spread(ocean[:, pl.ds(b * block_len, block_len)], HALO + b, 0)
    slot = atm_owner[...]
    away = (slot // owned) ^ me
    ranks = []
    for bits in bits_of:
        rank = away * 0
        for bit in bits:
            rank = rank * 2 + ((away >> bit) & 1)
        ranks.append(rank * owned + slot % owned)
    ocean_copy.wait_recv()
    for b in range(nblocks):
        spread(other[:, pl.ds(b * block_len, block_len)], HALO + b, 1)
    atm_copy.wait_recv()
    atm_tiles = atm_owner.shape[1]
    ids = lax.broadcasted_iota(jnp.int32, (atm_tiles, tiles), 0)
    tile_hot = jnp.concatenate(
        [
            (ids == tile_atm[...]).astype(jnp.float32),
            (ids == other_atm[...]).astype(jnp.float32),
        ],
        axis=1,
    ).astype(jnp.bfloat16)
    for kind, rel in enumerate(ranks):
        owner_hot = (
            (lax.broadcasted_iota(jnp.int32, (rows, atm_tiles), 0) == rel)
            .astype(jnp.float32)
            .astype(jnp.bfloat16)
        )
        chosen = jnp.dot(owner_hot, tile_hot, preferred_element_type=jnp.float32)
        select[kind, :, : 2 * tiles] = chosen.astype(jnp.bfloat16)
        select[kind, :, 2 * tiles :] = chosen[:, :tiles].astype(jnp.bfloat16)

    @pl.when(has_right)
    def _():
        for g in range(2):
            left_copies[g].wait_recv()
            for b in range(HALO):
                spread(halo[1, g, :, pl.ds(b * block_len, block_len)], HALO + nblocks + b, g)

    @pl.when(has_left)
    def _():
        for g in range(2):
            right_copies[g].wait_recv()
            for b in range(HALO):
                spread(halo[0, g, :, pl.ds(b * block_len, block_len)], b, g)

    base = me * nblocks
    for i in range(gw_parts):
        gw_copies[i].wait()

        def gradient(j, _, i=i):
            b = i * gw_step + j
            picked = [ext[jnp.clip(neighbours[k, b] - base + HALO, 0, nblocks + 2 * HALO - 1)] for k in range(stencil)]
            weights = gw[b].reshape(stencil * block_len, grad_len)
            grad = jnp.dot(
                jnp.concatenate(picked, axis=1), weights, preferred_element_type=jnp.float32
            )
            source[b, :, :block_len] = ext[HALO + b]
            source[b, :, block_len:] = grad.astype(jnp.bfloat16)
            return 0

        lax.fori_loop(0, gw_step, gradient, 0, unroll=True)

    part_copies = []
    loads_per = rw_parts // c_parts
    for i in range(c_parts):
        for j in range(loads_per):
            rw_copies[i * loads_per + j].wait()

        def contribute(j, _, i=i):
            t = i * c_step + j
            value = jnp.dot(
                source[jnp.clip(tile_src[t] - base, 0, nblocks - 1)], rw[t], preferred_element_type=jnp.float32
            )
            own_part[pl.ds(t * half_rows, half_rows), :] = value[:half_rows]
            send_part[t] = value[half_rows:].astype(jnp.bfloat16)
            return 0

        lax.fori_loop(0, c_step, contribute, 0, unroll=8)
        copy = remote(
            send_part.at[pl.ds(i * c_step, c_step)],
            recv_part.at[pl.ds(i * c_step, c_step)],
            part_send.at[i], part_recv.at[i], peer,
        )
        copy.start()
        part_copies.append(copy)

    for f in range(fields):
        g, at = f // (fields // groups), f % (fields // groups)
        mine = own_part[pl.ds(f, tiles, stride=half_rows), :]
        high = mine.astype(jnp.bfloat16)
        low = (mine - high.astype(jnp.float32)).astype(jnp.bfloat16)
        rhs[g, :tiles, at * cells : (at + 1) * cells] = high
        rhs[g, 2 * tiles :, at * cells : (at + 1) * cells] = low
    for i in range(c_parts):
        part_copies[i].wait_recv()
        own_part[pl.ds((tiles + i * c_step) * half_rows, c_step * half_rows), :] = (
            recv_part[pl.ds(i * c_step, c_step)]
            .astype(jnp.float32)
            .reshape(c_step * half_rows, cells)
        )

    def reduction(g, s):
        part = rows >> (s + 1)
        return remote(
            outgoing.at[g, pl.ds(part, part)], incoming.at[g, pl.ds(part, part)],
            red_send.at[g, s], red_recv.at[g, s], (me ^ (1 << bits_of[kinds[g]][s]), core),
        )

    per = fields // groups
    for g in range(groups):
        for at in range(per):
            theirs = own_part[pl.ds(tiles * half_rows + g * per + at, tiles, stride=half_rows), :]
            rhs[g, tiles : 2 * tiles, at * cells : (at + 1) * cells] = theirs.astype(jnp.bfloat16)
        outgoing[g, rows // 2 :] = jnp.dot(
            select[kinds[g], rows // 2 :], rhs[g], preferred_element_type=jnp.float32
        ).astype(jnp.bfloat16)
        reduction(g, 0).start()
    for g in range(groups):
        acc[g] = jnp.dot(
            select[kinds[g], : rows // 2], rhs[g], preferred_element_type=jnp.float32
        )
    steps = [(g, s) for s in range(stages) for g in range(groups)]
    for g, s in sorted(steps, key=lambda step: (step[0] + 2.5 * step[1], step[1])):
        part = rows >> (s + 1)
        reduction(g, s).wait_recv()
        if s < stages - 1:
            quarter = part // 2
            outgoing[g, quarter:part] = (
                acc[g, quarter:part] + incoming[g, part + quarter : 2 * part].astype(jnp.float32)
            ).astype(jnp.bfloat16)
            reduction(g, s + 1).start()
            acc[g, :quarter] += incoming[g, part : part + quarter].astype(jnp.float32)
        else:
            final = acc[g, :part] + incoming[g, part : 2 * part].astype(jnp.float32)
            for at in range(per):
                turned[pl.ds((g * per + at) * owned, owned), :] = final[
                    :, at * cells : (at + 1) * cells
                ]
    for a in range(owned):
        out[:, pl.ds(a * cells, cells)] = turned[pl.ds(a, fields, stride=owned), :]

    @pl.when(has_left)
    def _():
        for copy in left_copies:
            copy.wait_send()

    @pl.when(has_right)
    def _():
        for copy in right_copies:
            copy.wait_send()

    ocean_copy.wait_send()
    atm_copy.wait_send()
    for copy in part_copies:
        copy.wait_send()
    for s in range(stages):
        for g in range(groups):
            reduction(g, s).wait_send()


def fused(ocean, grad_weight, neighbours, remap_weight, tile_src, tile_atm, atm_owner):
    fields, width = ocean.shape
    devices = lax.axis_size("dom")
    stages = devices.bit_length() - 1
    nblocks, _, block_len, grad_len = grad_weight.shape
    tiles, depth, cells = remap_weight.shape
    owned = atm_owner.shape[0] // devices
    rows = devices * owned
    groups = 3 if fields % 3 == 0 else 1
    span = fields // groups * cells
    half = -(-fields // 16) * 16
    kinds = 1 + max(kind_of(g, groups, stages) for g in range(groups))
    bf16, f32 = jnp.bfloat16, jnp.float32
    dma = pltpu.SemaphoreType.DMA
    vmem = pl.BlockSpec(memory_space=pltpu.VMEM)
    smem = pl.BlockSpec(memory_space=pltpu.SMEM)
    anyspace = pl.BlockSpec(memory_space=pl.ANY)
    return pl.pallas_call(
        functools.partial(fused_kernel, devices, stages, owned, groups),
        out_shape=jax.ShapeDtypeStruct((fields, owned * cells), f32),
        in_specs=[vmem, smem, smem, vmem, vmem, anyspace, anyspace],
        out_specs=vmem,
        scratch_shapes=[
            pltpu.VMEM(grad_weight.shape, bf16),
            pltpu.VMEM(remap_weight.shape, bf16),
            pltpu.VMEM((fields, width), bf16),
            pltpu.VMEM((2, 2, fields, HALO * block_len), bf16),
            pltpu.VMEM((1, tiles), jnp.int32),
            pltpu.VMEM((nblocks + 2 * HALO, 2 * half, block_len), bf16),
            pltpu.VMEM((nblocks, 2 * half, depth), bf16),
            pltpu.VMEM((2 * tiles * half, cells), f32),
            pltpu.VMEM((tiles, half, cells), bf16),
            pltpu.VMEM((tiles, half, cells), bf16),
            pltpu.VMEM((kinds, rows, 3 * tiles), bf16),
            pltpu.VMEM((groups, 3 * tiles, span), bf16),
            pltpu.VMEM((groups, rows // 2, span), f32),
            pltpu.VMEM((groups, rows, span), bf16),
            pltpu.VMEM((groups, rows, span), bf16),
            pltpu.VMEM((fields * owned, cells), f32),
            dma((4,)), dma((8,)), dma((6,)), dma((6,)), dma((4,)), dma((4,)),
            dma((groups, stages)), dma((groups, stages)),
        ],
        compiler_params=pltpu.CompilerParams(
            collective_id=0, has_side_effects=True, vmem_limit_bytes=60 * 2**20
        ),
    )(
        ocean, neighbours.T, tile_src, tile_atm.reshape(1, -1), atm_owner.reshape(1, -1),
        grad_weight, remap_weight,
    )


def plan(ocean, grad_weight, neighbours, remap_weight, tile_src, tile_atm, atm_owner):
    devices = lax.axis_size("dom")
    atm_tiles = atm_owner.shape[0]
    power = devices > 1 and devices & (devices - 1) == 0
    small = atm_tiles * ocean.shape[0] * remap_weight.shape[2] <= 2**20
    even = (atm_tiles // devices) % 16 == 0 and lax.axis_size("field") == 2
    body = fused if power and small and even else local
    return body(ocean, grad_weight, neighbours, remap_weight, tile_src, tile_atm, atm_owner)


def solution(mesh):
    in_specs = (
        P("field", "dom"),
        P("dom", None, None, None),
        P("dom", None),
        P(("dom", "field"), None, None),
        P(("dom", "field")),
        P(("dom", "field")),
        P(),
    )
    out_specs = P("field", "dom")
    return jax.shard_map(plan, mesh=mesh, in_specs=in_specs, out_specs=out_specs, check_vma=False)
```
